32 devices in a mesh: row: 4 (over x, core), col: 8 (over z, y).
Axes of the slice: x: 2, y: 2, z: 4, core: 2. Of those that a mesh axis runs over, the one named last changes fastest.
Arguments:
- factor: float32 [1, 8192, 512], P(None, ('row', 'col')), may hold values from -40 to 40, as said below
- update: float32 [1, 8192, 256], P(None, ('row', 'col')), may hold values from -1.5 to 1.5
Outputs:
- new_factor: float32 [1, 8192, 512], P(None, ('row', 'col'))
- new_update: float32 [1, 8192, 256], P(None, ('row', 'col'))
- column_scale: float32 [512], replicated
The draws below stay inside these ranges and needn't reach their ends.
Inputs may be any that keep to these rules, and one draw needn't show every extreme that they name: `factor`: in the columns of panel p, rows of global tiles before p are zero; the diagonal block of panel p is lower triangular with diagonal entries of 1 to 2.
All inputs are finite; a program needn't handle non-finite values.
Results may differ from the reference program's by a relative error of at most 0.0003.
Values sent between devices are 32-bit elements; how exact they have to be, the bound alone decides.
No kernel may reach another device: no remote copies, remote signals or barrier semaphores. Data moves between devices by JAX's collectives and lax.ppermute only.
A program may use at most 64 MiB of HBM per device.

```python
import math
import jax
import jax.numpy as jnp
from jax import lax

PW = 256
K = 256
PANELS = 2
TILES_DEV = 1
N_ROW = 4
N_COL = 8


def draw_factor(key, part):
    devices = N_ROW * N_COL
    row_count = devices * PW
    col_count = PANELS * PW
    shape = (TILES_DEV, row_count, col_count)
    subkeys = jax.random.split(key, 5)
    values = jnp.clip(jax.random.normal(subkeys[0], shape, jnp.float32), -4.0, 4.0)
    spread = 0.9
    row_scale = jnp.exp(jax.random.uniform(subkeys[1], (TILES_DEV, row_count, 1), jnp.float32, -spread, spread))
    tile_index = lax.broadcasted_iota(jnp.int32, (TILES_DEV, row_count, 1), 0) * devices + lax.broadcasted_iota(jnp.int32, (TILES_DEV, row_count, 1), 1) // PW
    rising = 1.0 + 2.0 * tile_index.astype(jnp.float32) / max(TILES_DEV * devices - 1, 1)
    trailing = 0.5 * values * row_scale * rising
    panel_index = lax.broadcasted_iota(jnp.int32, (1, 1, col_count), 2) // PW
    inner_row = lax.broadcasted_iota(jnp.int32, (1, row_count, 1), 1) % PW
    inner_col = lax.broadcasted_iota(jnp.int32, (1, 1, col_count), 2) % PW
    diag_values = 1.0 + jax.random.uniform(subkeys[2], shape, jnp.float32)
    below_diag = 0.5 / math.sqrt(PW) * jnp.clip(jax.random.normal(subkeys[4], shape, jnp.float32), -4.0, 4.0)
    diag_block = jnp.where(inner_row > inner_col, below_diag, jnp.where(inner_row == inner_col, diag_values, 0.0))
    return jnp.where(tile_index < panel_index, 0.0, jnp.where(tile_index == panel_index, diag_block, trailing))


def level_of(own_key, extent, shards, least, top_value):
    loudness = 1.0
    for axis_at, parts in shards:
        steps = jax.random.uniform(jax.random.fold_in(jax.random.fold_in(own_key, 6), axis_at), (parts,), jnp.float32, least / len(shards), top_value / len(shards))
        loudness = loudness * jnp.repeat(jnp.exp(steps), extent[axis_at] // parts).reshape((-1,) + (1,) * (len(extent) - 1 - axis_at))
    return loudness


def scatter_about(stream_key, dims, scale, most, pieces=(), held_as=jnp.bfloat16):
    factor_of = level_of(stream_key, dims, pieces, -0.22, 0.18) if pieces else 1.0
    values = jax.random.normal(stream_key, dims, jnp.float32) * scale * factor_of
    return jnp.minimum(jnp.maximum(values, -most), most).astype(held_as)


def setup_inputs(seed: int = 0) -> dict:
    streams_of = jax.random.split(jax.random.key(seed), 3)
    return {
        "factor": draw_factor(jax.random.fold_in(streams_of[2], 71), 0),
        "update": scatter_about(streams_of[1], (TILES_DEV, N_ROW * N_COL * PW, K), 0.25, 1.5, ((1, 32),), jnp.float32),
    }


def panel_terms(block_factor, block_update):
    highest = lax.Precision.HIGHEST
    gram_matrix = jnp.dot(block_factor, block_factor.T, precision=highest) + jnp.dot(block_update, block_update.T, precision=highest)
    diag_new = jnp.linalg.cholesky(gram_matrix)
    solved = lax.linalg.triangular_solve(block_factor, block_update, left_side=True, lower=True)
    inner_matrix = jnp.eye(K, dtype=jnp.float32) + jnp.dot(solved.T, solved, precision=highest)
    chol_inner = jnp.linalg.cholesky(inner_matrix)
    left_first = lax.linalg.triangular_solve(diag_new, block_factor, left_side=True, lower=True).T
    left_second = lax.linalg.triangular_solve(diag_new, block_update, left_side=True, lower=True).T
    right_first = lax.linalg.triangular_solve(chol_inner, jnp.eye(K, dtype=jnp.float32), left_side=True, lower=True).T
    right_second = jnp.dot(solved, right_first, precision=highest)
    return (left_first, left_second, right_first, right_second)

def reference(factor, update):
    highest = lax.Precision.HIGHEST
    width_all = factor.shape[2]
    flat_factor = factor.reshape(-1, width_all)
    current = update.reshape(-1, K)
    row_total = flat_factor.shape[0]
    columns_out = []
    for panel_num in range(PANELS):
        low = panel_num * PW
        panel_cols = flat_factor[:, low:low + PW]
        block_factor = panel_cols[low:low + PW]
        block_update = current[low:low + PW]
        left_first, left_second, right_first, right_second = panel_terms(block_factor, block_update)
        columns_out.append(jnp.dot(panel_cols, left_first, precision=highest) + jnp.dot(current, left_second, precision=highest))
        current = jnp.dot(current, right_first, precision=highest) - jnp.dot(panel_cols, right_second, precision=highest)
    new_cols = jnp.concatenate(columns_out, axis=1)
    column_scale = jnp.sqrt(lax.optimization_barrier(jnp.sum(new_cols * new_cols, axis=0)) / row_total + 1e-06)
    return (new_cols.reshape(factor.shape), current.reshape(update.shape), column_scale)
```

```python
import jax
import jax.numpy as jnp
from jax import lax
from jax.experimental import pallas as pl
from jax.experimental.pallas import tpu as pltpu
from jax.sharding import PartitionSpec as P

T = 8
N = 128
NB = N // T
AXES = ("row", "col")
HI = lax.Precision.HIGHEST
F32 = jnp.float32


def dot(a, b, ca, cb):
    return lax.dot_general(a, b, (((ca,), (cb,)), ((), ())), precision=HI, preferred_element_type=F32)


def mm(a, b):
    return dot(a, b, 1, 0)


def mm_nt(a, b):
    return dot(a, b, 1, 1)


def mm_tn(a, b):
    return dot(a, b, 0, 0)


def lane_bcast(x, lane):
    return jnp.broadcast_to(x[:, lane : lane + 1], (T, N))


def row_bcast(ref, row):
    return jnp.broadcast_to(ref[row : row + 1, :], (T, N))


def tiles_of(ref, start):
    return [ref[start + t * T : start + (t + 1) * T, start : start + N] for t in range(NB)]


def store_rows(out, start, k, rows, lane, sub):
    tile = rows[T - 1]
    for j in range(T - 2, -1, -1):
        tile = jnp.where(sub <= j, rows[j], tile)
    out[start + k : start + k + T, start : start + N] = jnp.where(lane <= sub + k, tile, 0.0)


def eliminate(mat, b, rows, inside):
    k = b * T
    for t in range(b + 1, NB):
        cur = mat[t]
        even = jnp.where(inside, 0.0, cur)
        odd = None
        for j in range(T):
            term = lane_bcast(cur, k + j) * rows[j]
            if j % 2 == 0:
                even = even - term
            else:
                odd = term if odd is None else odd + term
        mat[t] = even - odd


def chol_inverse(mats, outs, start, cols, rows_ref):
    lane = lax.broadcasted_iota(jnp.int32, (T, N), 1)
    sub = lax.broadcasted_iota(jnp.int32, (T, N), 0)
    for b in range(NB):
        k = b * T
        inside = (lane >= k) & (lane < k + T)
        unit = (lane == sub + k).astype(F32)
        for q, mat in enumerate(mats):
            sc = cols.at[q, b % 2]
            sr = rows_ref.at[q, b % 2]
            own = mat[b]
            for j in range(T):
                sc[j * T : (j + 1) * T, :] = lane_bcast(own, k + j)
            sr[...] = jnp.where(inside, unit, own)
            a = {(i, j): row_bcast(sc, j * T + i) for j in range(T) for i in range(j, T)}
            r = [row_bcast(sr, j) for j in range(T)]
            low = {}
            inv = []
            for j in range(T):
                scale = lax.rsqrt(a[j, j])
                inv.append(scale)
                for i in range(j + 1, T):
                    low[i, j] = a[i, j] * scale
                for i in range(j + 1, T):
                    for i2 in range(j + 1, i + 1):
                        a[i, i2] = a[i, i2] - low[i, j] * low[i2, j]
                r[j] = r[j] * scale
                for i in range(j + 1, T):
                    r[i] = r[i] - low[i, j] * r[j]
            store_rows(outs[q], start, k, r, lane, sub)
            if b < NB - 1:
                for j in range(T - 1, -1, -1):
                    r[j] = r[j] * inv[j]
                    for i in range(j):
                        r[i] = r[i] - low[j, i] * r[j]
                eliminate(mat, b, r, inside)


def tri_inverse(mats, outs, start, cols, rows_ref):
    lane = lax.broadcasted_iota(jnp.int32, (T, N), 1)
    sub = lax.broadcasted_iota(jnp.int32, (T, N), 0)
    for b in range(NB):
        k = b * T
        inside = (lane >= k) & (lane < k + T)
        unit = (lane == sub + k).astype(F32)
        for q, mat in enumerate(mats):
            sc = cols.at[q, b % 2]
            sr = rows_ref.at[q, b % 2]
            own = mat[b]
            for j in range(T):
                sc[j * T : (j + 1) * T, :] = lane_bcast(own, k + j)
            sr[...] = jnp.where(inside, unit, jnp.where(lane < k, own, 0.0))
            r = [row_bcast(sr, j) for j in range(T)]
            for j in range(T):
                r[j] = r[j] * (1.0 / row_bcast(sc, j * T + j))
                for i in range(j + 1, T):
                    r[i] = r[i] - row_bcast(sc, j * T + i) * r[j]
            store_rows(outs[q], start[q], k, r, lane, sub)
            eliminate(mat, b, r, inside)


def solve_kernel(mine, factor, update, solved, carried, inverse, cols, rows_ref):
    width = update.shape[1]
    low = pl.multiple_of(mine[0] * width, width)
    block = factor.at[:, pl.ds(low, width)]
    tri_inverse(
        [tiles_of(block, 0), tiles_of(block, N)], [inverse, inverse], [0, N], cols, rows_ref
    )
    upper = inverse[:N, :N]
    lower = inverse[N:, N:]
    corner = block[N:, :N]
    for rhs, out in ((update, solved), (factor.at[:, :width], carried)):
        top = mm(upper, rhs[:N, :])
        out[:N, :] = top
        out[N:, :] = mm(lower, rhs[N:, :] - mm(corner, top))


def both_inverses(grams, inverses, cols, rows_ref):
    chol_inverse([tiles_of(g, 0) for g in grams], inverses, 0, cols, rows_ref)
    corners = []
    for gram, inv in zip(grams, inverses):
        corner = mm_nt(gram[N:, :N], inv[:N, :N])
        gram[N:, N:] = gram[N:, N:] - mm_nt(corner, corner)
        corners.append(mm(corner, inv[:N, :N]))
    chol_inverse([tiles_of(g, N) for g in grams], inverses, N, cols, rows_ref)
    for inv, corner in zip(inverses, corners):
        inv[N:, :N] = -mm(inv[N:, N:], corner)
        inv[:N, N:] = jnp.zeros((N, N), F32)


def update_kernel(
    factor, update, first, second, carried, new_factor, new_update, sums,
    gram_l, gram_c, inv_l, inv_c, current, solved, mixed, cols, rows_ref,
):
    width = update.shape[1]
    panels = factor.shape[1] // width
    eye = (
        lax.broadcasted_iota(jnp.int32, (width, width), 0)
        == lax.broadcasted_iota(jnp.int32, (width, width), 1)
    ).astype(F32)
    current[...] = update[...]
    solved[...] = first[...]
    sums[...] = jnp.zeros(sums.shape, F32)
    for p in range(panels):
        columns = slice(p * width, (p + 1) * width)
        g = solved[...]
        gram_l[...] = eye + mm_nt(g, g)
        gram_c[...] = eye + mm_tn(g, g)
        mixed[...] = factor[:, columns] + mm_nt(current[...], g)
        current[...] = current[...] - mm(factor[:, columns], g)
        if p == 0:
            solved[...] = second[...] - mm(carried[...], g)
        both_inverses([gram_l, gram_c], [inv_l, inv_c], cols, rows_ref)
        cols_out = mm_nt(mixed[...], inv_l[...])
        new_factor[:, columns] = cols_out
        squares = jnp.sum(cols_out * cols_out, axis=0, keepdims=True)
        for c in range(width // N):
            sums[p * (width // N) + c : p * (width // N) + c + 1, :] = squares[:, c * N : (c + 1) * N]
        current[...] = mm_nt(current[...], inv_c[...])
        if p == 0:
            solved[...] = mm_nt(solved[...], inv_c[...])
    new_update[...] = current[...]


def masks_of(rows, cols):
    core = cols if rows > 1 else 0
    others = []
    bit = 1
    while bit < cols:
        others.append(bit if bit < 4 else bit | (bit >> 1))
        bit *= 2
    bit = 2 * cols
    while bit < rows * cols:
        others.append(bit)
        bit *= 2
    return core, others


def spread(held, core, others, my_index, total):
    half = held.shape[0] // 2
    mine = jnp.where((my_index & core) == 0, held[:half], held[half:])
    sent = lax.ppermute(held[half:], AXES, [(0, core), (1, 1 | core)])
    part = jnp.where(my_index < 2, held[:half], sent)
    steps = others[1:]
    turned = steps[1:] + steps[:1]
    seen = [{0, 1}, {core, 1 | core}]
    for step in range(len(steps)):
        pairs = []
        for side, order in ((0, steps), (1, turned)):
            new = {(d, d ^ order[step]) for d in seen[side]}
            pairs += sorted(new)
            seen[side] |= {d for _, d in new}
        got = lax.ppermute(part, AXES, pairs)
        target = jnp.zeros((), bool)
        for _, d in pairs:
            target = target | (my_index == d)
        part = jnp.where(target, got, part)
    other = lax.ppermute(part, AXES, [(d, d ^ 1) for d in range(total)])
    odd = (my_index & 1) == 1
    both = jnp.concatenate([jnp.where(odd, other, part), jnp.where(odd, part, other)], axis=0)
    swapped = lax.ppermute(both, AXES, [(d, d ^ core) for d in range(total)])
    south = (my_index & core) != 0
    a, b = jnp.where(south, swapped, both), jnp.where(south, both, swapped)
    return (
        jnp.concatenate([a[:half], b[:half]], axis=0),
        jnp.concatenate([a[half:], b[half:]], axis=0),
    )


def on_device(factor, update):
    rows, cols_count = lax.axis_size("row"), lax.axis_size("col")
    total = rows * cols_count
    my_index = lax.axis_index(AXES)
    tile, wide = factor.shape[1], factor.shape[2]
    width = update.shape[2]
    panels = wide // width
    flat_factor = factor.reshape(tile, wide)
    flat_update = update.reshape(tile, width)
    square = jax.ShapeDtypeStruct((width, width), F32)
    vmem = pl.BlockSpec(memory_space=pltpu.VMEM)
    scratch = [pltpu.VMEM((2, 2, T * T, N), F32), pltpu.VMEM((2, 2, T, N), F32)]
    solved, carried = pl.pallas_call(
        solve_kernel,
        out_shape=(square, square),
        in_specs=[pl.BlockSpec(memory_space=pltpu.SMEM), vmem, vmem],
        out_specs=(vmem, vmem),
        scratch_shapes=[pltpu.VMEM((width, width), F32)] + scratch,
        name="solve",
    )(jnp.minimum(my_index, panels - 1).reshape(1), flat_factor, flat_update)
    core, others = masks_of(rows, cols_count)
    first, second = spread(solved, core, others, my_index, total)
    _, carried = spread(carried, core, others, my_index, total)
    big = lambda: pltpu.VMEM((width, width), F32)
    new_factor, new_update, sums = pl.pallas_call(
        update_kernel,
        out_shape=(
            jax.ShapeDtypeStruct((tile, wide), F32),
            jax.ShapeDtypeStruct((tile, width), F32),
            jax.ShapeDtypeStruct((T, N), F32),
        ),
        in_specs=[vmem] * 5,
        out_specs=(vmem,) * 3,
        scratch_shapes=[big() for _ in range(7)] + scratch,
        name="update",
    )(flat_factor, flat_update, first, second, carried)
    copies = jnp.broadcast_to(sums[None], (total, T, N)).reshape(total * T, N)
    gathered = lax.all_to_all(copies, AXES, 0, 0, tiled=True)
    squares = jnp.sum(gathered.reshape(total, T, N), axis=0)[: wide // N].reshape(wide)
    column_scale = jnp.sqrt(squares / (tile * total) + 1e-06)
    return (new_factor.reshape(factor.shape), new_update.reshape(update.shape), column_scale)


def solution(mesh):
    return jax.shard_map(
        on_device,
        mesh=mesh,
        in_specs=(P(None, AXES, None), P(None, AXES, None)),
        out_specs=(P(None, AXES, None), P(None, AXES, None), P()),
        check_vma=False,
    )
```

```python
import jax
import jax.numpy as jnp
from jax import lax
from jax.experimental import pallas as pl
from jax.experimental.pallas import tpu as pltpu
from jax.sharding import PartitionSpec as P

T = 8
N = 128
H = N // 2
NB = H // T
AXES = ("row", "col")
F32 = jnp.float32
HI = lax.Precision.HIGHEST

def dot(a, b, ca, cb):
    return lax.dot_general(a, b, (((ca,), (cb,)), ((), ())), precision=HI, preferred_element_type=F32)

def mm(a, b):
    return dot(a, b, 1, 0)

def mm_nt(a, b):
    return dot(a, b, 1, 1)

def mm_tn(a, b):
    return dot(a, b, 0, 0)

def half_masks():
    lane = lax.broadcasted_iota(jnp.int32, (T, N), 1)
    sub = lax.broadcasted_iota(jnp.int32, (T, N), 0)
    left = lane < H
    return jnp.where(left, lane, lane - H), sub, jnp.where(left, 0, H)

def pick(x, base, c):
    return jnp.take_along_axis(x, base + c, axis=1, mode="promise_in_bounds")

def row_bcast(ref, row):
    return jnp.broadcast_to(ref[row : row + 1, :], (T, N))

def assemble(rows, k, col, sub):
    tile = rows[T - 1]
    for j in range(T - 2, -1, -1):
        tile = jnp.where(sub <= j, rows[j], tile)
    return jnp.where(col <= sub + k, tile, 0.0)

def chol_leaf(mat, sc, sl, sr):
    col, sub, base = half_masks()
    mat = list(mat)
    out = []
    own = [pick(mat[0], base, j) for j in range(T)]
    for b in range(NB):
        k = b * T
        inside = (col >= k) & (col < k + T)
        unit = (col == sub + k).astype(F32)
        cs, ls, rs = sc.at[b % 2], sl.at[b % 2], sr.at[b % 2]
        for j in range(T):
            cs[j * T : (j + 1) * T, :] = own[j]
        rs[...] = jnp.where(inside, unit, mat[b])
        a = {(i, j): row_bcast(cs, j * T + i) for j in range(T) for i in range(j, T)}
        r = [row_bcast(rs, j) for j in range(T)]
        below = range(b + 1, NB)
        c = {t: [pick(mat[t], base, k + j) for j in range(T)] for t in below}
        if b < NB - 1:
            own = [pick(mat[b + 1], base, k + T + j) for j in range(T)]
        acc = {t: jnp.where(inside, 0.0, mat[t]) for t in below}
        for j in range(T):
            scale = lax.rsqrt(a[j, j])
            low = {i: a[i, j] * scale for i in range(j + 1, T)}
            for i in range(j + 1, T):
                for i2 in range(j + 1, i + 1):
                    a[i, i2] = a[i, i2] - low[i] * low[i2]
            r[j] = r[j] * scale
            for i in range(j + 1, T):
                r[i] = r[i] - low[i] * r[j]
            for t in below:
                c[t][j] = c[t][j] * scale
                for i in range(j + 1, T):
                    c[t][i] = c[t][i] - low[i] * c[t][j]
                acc[t] = acc[t] - c[t][j] * r[j]
            if b < NB - 1:
                ls[j * T : (j + 1) * T, :] = c[b + 1][j]
                for i in range(T):
                    own[i] = own[i] - c[b + 1][j] * row_bcast(ls, j * T + i)
        out.append(assemble(r, k, col, sub))
        for t in below:
            mat[t] = acc[t]
    return out

def tri_leaf(mats, scs, srs):
    col, sub, base = half_masks()
    mats = [list(m) for m in mats]
    outs = [[] for _ in mats]
    picks = []
    for mat, sc in zip(mats, scs):
        picks.append([{t: [pick(mat[t], base, b * T + j) for j in range(T)] for t in range(b, NB)} for b in range(NB)])
        for b in range(NB):
            for j in range(T):
                sc[b, j * T : (j + 1) * T, :] = picks[-1][b][b][j]
    mats = [[jnp.zeros((T, N), F32) for _ in m] for m in mats]
    for b in range(NB):
        k = b * T
        inside = (col >= k) & (col < k + T)
        unit = (col == sub + k).astype(F32)
        for q, mat in enumerate(mats):
            cs, rs = scs[q].at[b], srs[q].at[b % 2]
            rs[...] = jnp.where(inside, unit, mat[b])
            r = [row_bcast(rs, j) for j in range(T)]
            for j in range(T):
                r[j] = r[j] * (1.0 / row_bcast(cs, j * T + j))
                for i in range(j + 1, T):
                    r[i] = r[i] - row_bcast(cs, j * T + i) * r[j]
            outs[q].append(assemble(r, k, col, sub))
            for t in range(b + 1, NB):
                for j in range(T):
                    mat[t] = mat[t] - picks[q][b][t][j] * r[j]
    return outs

def split_halves(x):
    lane = lax.broadcasted_iota(jnp.int32, x.shape, 1)
    return jnp.concatenate([jnp.where(lane < H, x, 0.0), jnp.where(lane < H, 0.0, x)], axis=0)

def pack(first, second):
    lane = lax.broadcasted_iota(jnp.int32, (first.shape[0], N), 1)
    out = []
    for c in range(0, first.shape[1], N):
        x, y = first[:, c : c + N], second[:, c : c + N]
        out.append(jnp.where(lane < H, x, pltpu.roll(y, H, 1)))
        out.append(jnp.where(lane < H, pltpu.roll(x, H, 1), y))
    return out

def tiles_of(ref, r0, c0):
    return [ref[r0 + t * T : r0 + (t + 1) * T, c0 : c0 + N] for t in range(NB)]

def chol_inverse_pair(gram, inv, tmp, sc, sl, sr):
    n = gram.shape[0]
    nb = n // H
    low = {}
    for d in range(nb):
        at = slice(d * H, (d + 1) * H)
        for t, tile in enumerate(chol_leaf(tiles_of(gram, d * H, d * N), sc, sl, sr)):
            inv[d * H + t * T : d * H + (t + 1) * T, d * N : (d + 1) * N] = tile
        w = inv[at, d * N : (d + 1) * N]
        if d < nb - 1:
            rest = slice((d + 1) * H, n)
            tmp[rest, d * N : (d + 1) * N] = mm_nt(gram[rest, d * N : (d + 1) * N], split_halves(w))
            for e in range(d + 1, nb):
                rows = slice(e * H, n)
                cols = slice(e * N, (e + 1) * N)
                gram[rows, cols] = gram[rows, cols] - mm_nt(
                    tmp[rows, d * N : (d + 1) * N], split_halves(tmp[e * H : (e + 1) * H, d * N : (d + 1) * N])
                )
        for c in range(d):
            cols = slice(c * N, (c + 1) * N)
            part = None
            for e in range(c, d):
                term = mm(tmp[at, e * N : (e + 1) * N], split_halves(inv[e * H : (e + 1) * H, cols]))
                part = term if part is None else part + term
            inv[at, cols] = -mm(w, split_halves(part))

def unpack(inv, first, second):
    n = inv.shape[0]
    lane = lax.broadcasted_iota(jnp.int32, (n, N), 1)
    row = lax.broadcasted_iota(jnp.int32, (n, N), 0)
    for c in range(0, n, N):
        x, y = inv[:, 2 * c : 2 * c + N], inv[:, 2 * c + N : 2 * c + 2 * N]
        x = jnp.where(row >= c, x, 0.0)
        y = jnp.where(row >= c + H, y, 0.0)
        first[:, c : c + N] = jnp.where(lane < H, x, pltpu.roll(y, H, 1))
        second[:, c : c + N] = jnp.where(lane < H, pltpu.roll(x, H, 1), y)

def tri_inverse(block, inverse, scs, srs):
    n = block.shape[0]
    lane = lax.broadcasted_iota(jnp.int32, (T, N), 1)
    mats = []
    for c in range(0, n, N):
        mats.append([
            jnp.where(lane < H, block[c + t * T : c + (t + 1) * T, c : c + N], block[c + H + t * T : c + H + (t + 1) * T, c : c + N])
            for t in range(NB)
        ])
    outs = tri_leaf(mats, scs, srs)
    for c, out in zip(range(0, n, N), outs):
        for t, tile in enumerate(out):
            inverse[c + t * T : c + (t + 1) * T, c : c + N] = jnp.where(lane < H, tile, 0.0)
            inverse[c + H + t * T : c + H + (t + 1) * T, c : c + N] = jnp.where(lane < H, 0.0, tile)
    big = lax.broadcasted_iota(jnp.int32, (H, N), 1)
    for c in range(0, n, N):
        diag = inverse[c : c + N, c : c + N]
        corner = jnp.where(big < H, block[c + H : c + N, c : c + N], 0.0)
        t1 = mm(corner, diag)
        t2 = mm(diag[H:, :], jnp.concatenate([jnp.zeros((H, N), F32), t1], axis=0))
        inverse[c + H : c + N, c : c + N] = diag[H:, :] - t2


def inverse_kernel(flags, factor, inverse, scs, srs):
    width = inverse.shape[0]
    block = factor.at[:, pl.ds(pl.multiple_of(flags[0] * width, width), width)]
    tri_inverse(block, inverse, [scs.at[q] for q in range(2)], [srs.at[q] for q in range(2)])


def solve_kernel(flags, factor, update, inverse, left, right, rhs):
    width = update.shape[1]
    half = width // 2
    block = factor.at[:, pl.ds(pl.multiple_of(flags[0] * width, width), width)]
    for c in range(0, width, N):
        at = slice(c, c + N)
        inv = inverse[at, at]
        for source, low in ((update, 0), (factor, width)):
            value = source[at, :width]
            if c > 0:
                value = value - mm(block[at, :c], rhs[:c, low : low + width])
            rhs[at, low : low + width] = mm(inv, value)
    for out, low in ((left, 0), (right, half)):
        out[:, :half] = rhs[:, low : low + half]
        out[:, half:] = rhs[:, width + low : width + low + half]


def panel_step(columns, current, g, new_columns, inv_l, inv_c, gram, inv, tmp, sc, sl, sr):
    width = g.shape[0]
    eye = (
        lax.broadcasted_iota(jnp.int32, (width, width), 0)
        == lax.broadcasted_iota(jnp.int32, (width, width), 1)
    ).astype(F32)
    x = g[...]
    for c, part in enumerate(pack(eye + mm_nt(x, x), eye + mm_tn(x, x))):
        gram[:, c * N : (c + 1) * N] = part
    cols = columns[...]
    v = current[...]
    new_columns[...] = cols + mm_nt(v, x)
    current[...] = v - mm(cols, x)
    chol_inverse_pair(gram, inv, tmp, sc, sl, sr)
    unpack(inv, inv_l, inv_c)
    new_columns[...] = mm_nt(new_columns[...], inv_l[...])
    current[...] = mm_nt(current[...], inv_c[...])


def update_kernel(
    flags, factor, update, own, other, own_swapped, other_swapped,
    new_factor, current, copies, g, x, inv_l, inv_c, *rest,
):
    width = g.shape[0]
    half = width // 2
    south = flags[1] == 1
    odd = flags[2] == 1

    def halves(low, swap):
        at = slice(low, low + half)
        here = jnp.where(odd != swap, other[:, at], own[:, at])
        there = jnp.where(odd != swap, other_swapped[:, at], own_swapped[:, at])
        return jnp.where(south, there, here), jnp.where(south, here, there)

    g[:, :half], g[:, half:] = halves(0, False)
    y = jnp.concatenate(halves(half, True), axis=1)
    x[...] = jnp.concatenate(halves(0, True), axis=1) - mm(y, g[...])
    current[...] = update[...]
    panel_step(factor.at[:, :width], current, g, new_factor.at[:, :width], inv_l, inv_c, *rest)
    x[...] = mm_nt(x[...], inv_c[...])
    panel_step(factor.at[:, width:], current, x, new_factor.at[:, width:], inv_l, inv_c, *rest)
    squares = jnp.sum(new_factor[...] * new_factor[...], axis=0, keepdims=True)
    sub = lax.broadcasted_iota(jnp.int32, (T, N), 0)
    tile = jnp.zeros((T, N), F32)
    for c in range(squares.shape[1] // N):
        tile = jnp.where(sub == c, squares[:, c * N : (c + 1) * N], tile)
    for d in range(copies.shape[0] // T):
        copies[d * T : (d + 1) * T, :] = tile


def masks_of(rows, cols):
    bits = lambda low, high: [1 << b for b in range(high.bit_length() - 2, low.bit_length() - 2, -1)]
    return cols, bits(2, cols) + bits(2 * cols, rows * cols)


def spread(left, right, my_index, core, steps, roots):
    turned = steps[-1:] + steps[:-1]
    sent = lax.ppermute(right, AXES, [(d, d | core) for d in roots])
    part = jnp.where((my_index & core) != 0, sent, left)
    seen = [set(roots), {core | d for d in roots}]
    for step in range(len(steps)):
        pairs = []
        for side, order in ((0, steps), (1, turned)):
            new = {(d, d ^ order[step]) for d in seen[side]}
            pairs += sorted(new)
            seen[side] |= {d for _, d in new}
        came = lax.ppermute(part, AXES, pairs)
        target = jnp.zeros((), bool)
        for _, d in pairs:
            target = target | (my_index == d)
        part = jnp.where(target, came, part)
    return part


def on_device(factor, update):
    rows, cols_count = lax.axis_size("row"), lax.axis_size("col")
    total = rows * cols_count
    my_index = lax.axis_index(AXES)
    tile, wide = factor.shape[1], factor.shape[2]
    width = update.shape[2]
    panels = wide // width
    flat_factor = factor.reshape(tile, wide)
    flat_update = update.reshape(tile, width)
    core, others = masks_of(rows, cols_count)
    panel = jnp.minimum(my_index & ~core, panels - 1)
    flags = jnp.stack([panel, jnp.minimum(my_index & core, 1), my_index & 1]).astype(jnp.int32)
    smem = pl.BlockSpec(memory_space=pltpu.SMEM)
    vmem = pl.BlockSpec(memory_space=pltpu.VMEM)
    shape = lambda *dims: jax.ShapeDtypeStruct(dims, F32)
    work = lambda *dims: pltpu.VMEM(dims, F32)
    limit = pltpu.CompilerParams(vmem_limit_bytes=24 * 2 ** 20)

    blocks = width // N
    inverse = pl.pallas_call(
        inverse_kernel,
        out_shape=shape(width, width),
        in_specs=[smem, vmem],
        out_specs=vmem,
        scratch_shapes=[work(blocks, NB, T * T, N), work(blocks, 2, T, N)],
        compiler_params=limit,
        name="inverse",
    )(flags, flat_factor)
    left, right = pl.pallas_call(
        solve_kernel,
        out_shape=(shape(width, width),) * 2,
        in_specs=[smem] + [vmem] * 3,
        out_specs=(vmem,) * 2,
        scratch_shapes=[work(width, 2 * width)],
        compiler_params=limit,
        name="solve",
    )(flags, flat_factor, flat_update, inverse)
    own = spread(left, right, my_index, core, others, (0, 1))
    partner = [(d, d ^ core) for d in range(total)]
    other = lax.ppermute(own, AXES, [(d, d ^ 1) for d in range(total)])
    own_swapped = lax.ppermute(own, AXES, partner)
    other_swapped = lax.ppermute(other, AXES, partner)
    new_factor, new_update, copies = pl.pallas_call(
        update_kernel,
        out_shape=(shape(tile, wide), shape(tile, width), shape(total * T, N)),
        in_specs=[smem] + [vmem] * 6,
        out_specs=(vmem,) * 3,
        scratch_shapes=[work(width, width)] * 4
        + [work(width, 2 * width)] * 3
        + [work(2, T * T, N), work(2, T * T, N), work(2, T, N)],
        compiler_params=limit,
        cost_estimate=pl.CostEstimate(flops=10 ** 10, bytes_accessed=2 ** 21, transcendentals=0),
        name="update",
    )(flags, flat_factor, flat_update, own, other, own_swapped, other_swapped)
    gathered = lax.all_to_all(copies, AXES, 0, 0, tiled=True)
    squares = jnp.sum(gathered.reshape(total, T, N), axis=0)[: wide // N].reshape(wide)
    column_scale = jnp.sqrt(squares / (tile * total) + 1e-06)
    return (new_factor.reshape(factor.shape), new_update.reshape(update.shape), column_scale)


def solution(mesh):
    return jax.shard_map(
        on_device,
        mesh=mesh,
        in_specs=(P(None, AXES, None), P(None, AXES, None)),
        out_specs=(P(None, AXES, None), P(None, AXES, None), P()),
        check_vma=False,
    )
```

```python
import jax
import jax.numpy as jnp
from jax import lax
from jax.experimental import pallas as pl
from jax.experimental.pallas import tpu as pltpu
from jax.sharding import PartitionSpec as P

T = 8
N = 128
H = N // 2
NB = H // T
SMALL = 32
AXES = ("row", "col")
F32 = jnp.float32
HI = lax.Precision.HIGHEST

def dot(a, b, ca, cb):
    return lax.dot_general(a, b, (((ca,), (cb,)), ((), ())), precision=HI, preferred_element_type=F32)

def mm(a, b):
    return dot(a, b, 1, 0)

def mm_nt(a, b):
    return dot(a, b, 1, 1)

def mm_tn(a, b):
    return dot(a, b, 0, 0)

def half_masks():
    lane = lax.broadcasted_iota(jnp.int32, (T, N), 1)
    sub = lax.broadcasted_iota(jnp.int32, (T, N), 0)
    left = lane < H
    return jnp.where(left, lane, lane - H), sub, jnp.where(left, 0, H)

def pick(x, base, c):
    return jnp.take_along_axis(x, base + c, axis=1, mode="promise_in_bounds")

def row_bcast(ref, row):
    return jnp.broadcast_to(ref[row : row + 1, :], (T, N))

def assemble(rows, k, col, sub):
    tile = rows[T - 1]
    for j in range(T - 2, -1, -1):
        tile = jnp.where(sub <= j, rows[j], tile)
    return jnp.where(col <= sub + k, tile, 0.0)

def chol_leaf(mat, sc, sl, sr, fill=()):
    fill = list(fill)
    rate = -(-len(fill) // NB)
    col, sub, base = half_masks()
    mat = list(mat)
    out = []
    own = [pick(mat[0], base, j) for j in range(T)]
    for b in range(NB):
        k = b * T
        inside = (col >= k) & (col < k + T)
        unit = (col == sub + k).astype(F32)
        cs, ls, rs = sc.at[b % 2], sl.at[b % 2], sr.at[b % 2]
        for j in range(T):
            cs[j * T : (j + 1) * T, :] = own[j]
        rs[...] = jnp.where(inside, unit, mat[b])
        a = {(i, j): row_bcast(cs, j * T + i) for j in range(T) for i in range(j, T)}
        r = [row_bcast(rs, j) for j in range(T)]
        below = range(b + 1, NB)
        c = {t: [pick(mat[t], base, k + j) for j in range(T)] for t in below}
        if b < NB - 1:
            own = [pick(mat[b + 1], base, k + T + j) for j in range(T)]
        acc = {t: jnp.where(inside, 0.0, mat[t]) for t in below}
        for task in fill[b * rate : (b + 1) * rate]:
            task()
        for j in range(T):
            scale = lax.rsqrt(a[j, j])
            low = {i: a[i, j] * scale for i in range(j + 1, T)}
            for i in range(j + 1, T):
                for i2 in range(j + 1, i + 1):
                    a[i, i2] = a[i, i2] - low[i] * low[i2]
            r[j] = r[j] * scale
            for i in range(j + 1, T):
                r[i] = r[i] - low[i] * r[j]
            for t in below:
                c[t][j] = c[t][j] * scale
                for i in range(j + 1, T):
                    c[t][i] = c[t][i] - low[i] * c[t][j]
                acc[t] = acc[t] - c[t][j] * r[j]
            if b < NB - 1:
                ls[j * T : (j + 1) * T, :] = c[b + 1][j]
                for i in range(T):
                    own[i] = own[i] - c[b + 1][j] * row_bcast(ls, j * T + i)
        out.append(assemble(r, k, col, sub))
        for t in below:
            mat[t] = acc[t]
    return out

def tri_leaf(mats, scs, srs):
    lane = lax.broadcasted_iota(jnp.int32, (T, N), 1)
    sub = lax.broadcasted_iota(jnp.int32, (T, N), 0)
    col = lane % SMALL
    base = lane - col
    count = SMALL // T
    outs = [[] for _ in mats]
    picks = []
    for mat, sc in zip(mats, scs):
        picks.append([{t: [pick(mat[t], base, b * T + j) for j in range(T)] for t in range(b, count)} for b in range(count)])
        for b in range(count):
            for j in range(T):
                sc[b, j * T : (j + 1) * T, :] = picks[-1][b][b][j]
    mats = [[jnp.zeros((T, N), F32) for _ in m] for m in mats]
    for b in range(count):
        k = b * T
        inside = (col >= k) & (col < k + T)
        unit = (col == sub + k).astype(F32)
        for q, mat in enumerate(mats):
            cs, rs = scs[q].at[b], srs[q].at[b % 2]
            rs[...] = jnp.where(inside, unit, mat[b])
            r = [row_bcast(rs, j) for j in range(T)]
            for j in range(T):
                r[j] = r[j] * (1.0 / row_bcast(cs, j * T + j))
                for i in range(j + 1, T):
                    r[i] = r[i] - row_bcast(cs, j * T + i) * r[j]
            outs[q].append(assemble(r, k, col, sub))
            for t in range(b + 1, count):
                for j in range(T):
                    mat[t] = mat[t] - picks[q][b][t][j] * r[j]
    return outs

def split_halves(x):
    lane = lax.broadcasted_iota(jnp.int32, x.shape, 1)
    return jnp.concatenate([jnp.where(lane < H, x, 0.0), jnp.where(lane < H, 0.0, x)], axis=0)

def pack(first, second):
    lane = lax.broadcasted_iota(jnp.int32, first.shape, 1)
    return (
        jnp.where(lane < H, first, pltpu.roll(second, H, 1)),
        jnp.where(lane < H, pltpu.roll(first, H, 1), second),
    )

def tiles_of(ref, r0, c0):
    return [ref[r0 + t * T : r0 + (t + 1) * T, c0 : c0 + N] for t in range(NB)]

def chol_inverse_pair(gram, inv, tmp, parts, sc, sl, sr, fills):
    n = gram.shape[0]
    nb = n // H
    rows = lambda e: slice(e * H, (e + 1) * H)
    cols = lambda e: slice(e * N, (e + 1) * N)
    span = lambda e, f: slice(e * N, f * N)
    pairs = lambda e, f: [(i, min(i + 2, f)) for i in range(e, f, 2)]

    def solve(d, at):
        tmp[at, cols(d)] = mm_nt(gram[at, cols(d)], split_halves(inv[rows(d), cols(d)]))

    def shrink(d, e, f, at):
        weights = jnp.concatenate([split_halves(tmp[rows(i), cols(d)]) for i in range(e, f)], axis=0)
        gram[at, span(e, f)] = gram[at, span(e, f)] - mm_nt(tmp[at, cols(d)], weights)

    def gather(d, e, f, c, b):
        weights = jnp.concatenate(
            [
                jnp.concatenate([split_halves(inv[rows(i), cols(k)]) for k in range(c, b)], axis=1)
                for i in range(e, f)
            ],
            axis=0,
        )
        part = mm(tmp[rows(d), span(e, f)], weights)
        parts[:, span(c, b)] = part if e == 0 else parts[:, span(c, b)] + part

    def finish(d, c, b):
        weights = jnp.concatenate([split_halves(parts[:, cols(k)]) for k in range(c, b)], axis=1)
        inv[rows(d), span(c, b)] = -mm(inv[rows(d), cols(d)], weights)

    inv[...] = jnp.zeros(inv.shape, F32)
    pending = []
    for d in range(nb):
        tasks = pending + [lambda e=e, f=f, c=c, b=b: gather(d, e, f, c, b) for e, f in pairs(0, d) for c, b in pairs(0, d)]
        tasks += fills.get(d, [])
        for t, tile in enumerate(chol_leaf(tiles_of(gram, d * H, d * N), sc, sl, sr, tasks)):
            inv[d * H + t * T : d * H + (t + 1) * T, cols(d)] = tile
        pending = []
        if d < nb - 1:
            solve(d, rows(d + 1))
            shrink(d, d + 1, d + 2, rows(d + 1))
            if d + 2 < nb:
                later = slice((d + 2) * H, n)
                pending.append(lambda d=d, at=later: solve(d, at))
                pending.append(lambda d=d, at=later: shrink(d, d + 1, d + 3, at))
            for e, f in pairs(d + 3, nb):
                pending.append(lambda d=d, e=e, f=f: shrink(d, e, f, slice(e * H, n)))
            pending += [lambda d=d, c=c, b=b: finish(d, c, b) for c, b in pairs(0, d)]
        else:
            for c, b in pairs(0, d):
                finish(d, c, b)

def unpack(inv, first, second):
    n = inv.shape[0]
    for c in range(0, n, N):
        first[:, c : c + N], second[:, c : c + N] = pack(inv[:, 2 * c : 2 * c + N], inv[:, 2 * c + N : 2 * c + 2 * N])

def tri_inverse(block, inverse, scs, srs):
    n = block.shape[0]
    lane = lax.broadcasted_iota(jnp.int32, (T, N), 1)
    mats = []
    for c in range(0, n, N):
        tiles = []
        for t in range(SMALL // T):
            tile = block[c + t * T : c + (t + 1) * T, c : c + N]
            for i in range(SMALL, N, SMALL):
                tile = jnp.where(lane < i, tile, block[c + i + t * T : c + i + (t + 1) * T, c : c + N])
            tiles.append(tile)
        mats.append(tiles)
    outs = tri_leaf(mats, scs, srs)
    row = lax.broadcasted_iota(jnp.int32, (N, N), 0)
    col = lax.broadcasted_iota(jnp.int32, (N, N), 1)
    for c, out in zip(range(0, n, N), outs):
        for i in range(0, N, SMALL):
            for t, tile in enumerate(out):
                inverse[c + i + t * T : c + i + (t + 1) * T, c : c + N] = jnp.where(
                    (lane >= i) & (lane < i + SMALL), tile, 0.0
                )
    for c in range(0, n, N):
        value = inverse[c : c + N, c : c + N]
        size = SMALL
        while size < N:
            corner = (row // size == col // size + 1) & (row // size % 2 == 1)
            value = value - mm(value, mm(jnp.where(corner, block[c : c + N, c : c + N], 0.0), value))
            size *= 2
        inverse[c : c + N, c : c + N] = value


def inverse_kernel(flags, factor, inverse, scs, srs):
    width = inverse.shape[0]
    block = factor.at[:, pl.ds(pl.multiple_of(flags[0] * width, width), width)]
    tri_inverse(block, inverse, [scs.at[q] for q in range(2)], [srs.at[q] for q in range(2)])


def solve_kernel(flags, factor, update, inverse, left, right, rhs):
    width = update.shape[1]
    half = width // 2
    block = factor.at[:, pl.ds(pl.multiple_of(flags[0] * width, width), width)]
    for c in range(0, width, N):
        at = slice(c, c + N)
        inv = inverse[at, at]
        for source, low in ((update, 0), (factor, width)):
            value = source[at, :width]
            if c > 0:
                value = value - mm(block[at, :c], rhs[:c, low : low + width])
            rhs[at, low : low + width] = mm(inv, value)
    for out, low in ((left, 0), (right, half)):
        out[:, :half] = rhs[:, low : low + half]
        out[:, half:] = rhs[:, width + low : width + low + half]


def gram_rows(g, gram, low, high, width):
    row = lax.broadcasted_iota(jnp.int32, (high - low, width), 0) + low
    eye = (row == lax.broadcasted_iota(jnp.int32, (high - low, width), 1)).astype(F32)
    first = eye + mm_nt(g[low:high, :], g[:width, :])
    left = g[:, :N] if high <= N else g[...]
    second = eye + mm_tn(left, g[:, :width])[low:high, :]
    for c in range(0, width, N):
        gram[low:high, 2 * c : 2 * c + N], gram[low:high, 2 * c + N : 2 * c + 2 * N] = pack(
            first[:, c : c + N], second[:, c : c + N]
        )


def update_kernel(
    flags, factor, update, own, other, own_swapped, other_swapped,
    new_factor, new_update, copies, g, x, y, mixed, current, inv_l, inv_c, gram, inv, tmp, parts, sc, sl, sr,
):
    width = g.shape[0]
    half = width // 2
    panels = factor.shape[1] // width
    south = flags[1] == 1
    odd = flags[2] == 1
    part = lambda p: slice(p * width, (p + 1) * width)

    def halves(out, low, swap):
        at = slice(low, low + half)
        here = jnp.where(odd != swap, other[:, at], own[:, at])
        there = jnp.where(odd != swap, other_swapped[:, at], own_swapped[:, at])
        out[:, :half] = jnp.where(south, there, here)
        out[:, half:] = jnp.where(south, here, there)

    def mix(p):
        v = update if p == 0 else new_update
        mixed[...] = factor[:, part(p)] + mm_nt(v[...], g[...])

    def lower(p):
        v = update if p == 0 else new_update
        current[...] = v[...] - mm(factor[:, part(p)], g[...])

    def carry():
        x[...] = x[...] - mm(y[...], g[...])

    def columns(p):
        new_factor[:, part(p)] = mm_nt(mixed[...], inv_l[...])

    def updates():
        new_update[...] = mm_nt(current[...], inv_c[...])

    halves(g, 0, False)
    halves(y, half, True)
    halves(x, 0, True)
    held = []
    for p in range(panels):
        gram_rows(g, gram, 0, H, N)
        rest = [lambda: gram_rows(g, gram, H, width, width)]
        tasks = {0: rest + held, 1: [lambda: mix(p), lambda: lower(p)], 2: [carry] if p < panels - 1 else []}
        chol_inverse_pair(gram, inv, tmp, parts, sc, sl, sr, tasks)
        unpack(inv, inv_l, inv_c)
        held = [lambda p=p: columns(p), updates]
        if p < panels - 1:
            g[...] = mm_nt(x[...], inv_c[...])
    for task in held:
        task()
    squares = jnp.sum(new_factor[...] * new_factor[...], axis=0, keepdims=True)
    copies[...] = jnp.broadcast_to(squares, copies.shape)


def masks_of(rows, cols):
    bits = lambda low, high: [1 << b for b in range(high.bit_length() - 2, low.bit_length() - 2, -1)]
    return cols, bits(2, cols) + bits(2 * cols, rows * cols)


def spread(left, right, my_index, core, steps, roots):
    turned = steps[-1:] + steps[:-1]
    sent = lax.ppermute(right, AXES, [(d, d | core) for d in roots])
    part = jnp.where((my_index & core) != 0, sent, left)
    seen = [set(roots), {core | d for d in roots}]
    for step in range(len(steps)):
        pairs = []
        for side, order in ((0, steps), (1, turned)):
            new = {(d, d ^ order[step]) for d in seen[side]}
            pairs += sorted(new)
            seen[side] |= {d for _, d in new}
        came = lax.ppermute(part, AXES, pairs)
        target = jnp.zeros((), bool)
        for _, d in pairs:
            target = target | (my_index == d)
        part = jnp.where(target, came, part)
    return part


def on_device(factor, update):
    rows, cols_count = lax.axis_size("row"), lax.axis_size("col")
    total = rows * cols_count
    my_index = lax.axis_index(AXES)
    tile, wide = factor.shape[1], factor.shape[2]
    width = update.shape[2]
    panels = wide // width
    flat_factor = factor.reshape(tile, wide)
    flat_update = update.reshape(tile, width)
    core, others = masks_of(rows, cols_count)
    panel = jnp.minimum(my_index & ~core, panels - 1)
    flags = jnp.stack([panel, jnp.minimum(my_index & core, 1), my_index & 1]).astype(jnp.int32)
    smem = pl.BlockSpec(memory_space=pltpu.SMEM)
    vmem = pl.BlockSpec(memory_space=pltpu.VMEM)
    shape = lambda *dims: jax.ShapeDtypeStruct(dims, F32)
    work = lambda *dims: pltpu.VMEM(dims, F32)
    limit = pltpu.CompilerParams(vmem_limit_bytes=24 * 2 ** 20)

    blocks = width // N
    inverse = pl.pallas_call(
        inverse_kernel,
        out_shape=shape(width, width),
        in_specs=[smem, vmem],
        out_specs=vmem,
        scratch_shapes=[work(blocks, NB, T * T, N), work(blocks, 2, T, N)],
        compiler_params=limit,
        name="inverse",
    )(flags, flat_factor)
    left, right = pl.pallas_call(
        solve_kernel,
        out_shape=(shape(width, width),) * 2,
        in_specs=[smem] + [vmem] * 3,
        out_specs=(vmem,) * 2,
        scratch_shapes=[work(width, 2 * width)],
        compiler_params=limit,
        name="solve",
    )(flags, flat_factor, flat_update, inverse)
    own = spread(left, right, my_index, core, others, (0, 1))
    partner = [(d, d ^ core) for d in range(total)]
    other = lax.ppermute(own, AXES, [(d, d ^ 1) for d in range(total)])
    own_swapped = lax.ppermute(own, AXES, partner)
    other_swapped = lax.ppermute(other, AXES, partner)
    new_factor, new_update, copies = pl.pallas_call(
        update_kernel,
        out_shape=(shape(tile, wide), shape(tile, width), shape(total, wide)),
        in_specs=[smem] + [vmem] * 6,
        out_specs=(vmem,) * 3,
        scratch_shapes=[work(width, width)] * 3
        + [work(tile, width)] * 2
        + [work(width, width)] * 2
        + [work(width, 2 * width)] * 3
        + [work(H, 2 * width), work(2, T * T, N), work(2, T * T, N), work(2, T, N)],
        compiler_params=limit,
        cost_estimate=pl.CostEstimate(flops=10 ** 10, bytes_accessed=2 ** 21, transcendentals=0),
        name="update",
    )(flags, flat_factor, flat_update, own, other, own_swapped, other_swapped)
    gathered = lax.all_to_all(copies, AXES, 0, 0, tiled=True)
    squares = jnp.sum(gathered, axis=0)
    column_scale = jnp.sqrt(squares / (tile * total) + 1e-06)
    return (new_factor.reshape(factor.shape), new_update.reshape(update.shape), column_scale)


def solution(mesh):
    return jax.shard_map(
        on_device,
        mesh=mesh,
        in_specs=(P(None, AXES, None), P(None, AXES, None)),
        out_specs=(P(None, AXES, None), P(None, AXES, None), P()),
        check_vma=False,
    )
```

```python
import jax
import jax.numpy as jnp
from jax import lax
from jax.experimental import pallas as pl
from jax.experimental.pallas import tpu as pltpu
from jax.sharding import PartitionSpec as P

T = 8
N = 128
H = N // 2
NB = H // T
SMALL = 32
AXES = ("row", "col")
F32 = jnp.float32
HI = lax.Precision.HIGHEST

def dot(a, b, ca, cb):
    return lax.dot_general(a, b, (((ca,), (cb,)), ((), ())), precision=HI, preferred_element_type=F32)

def mm(a, b):
    return dot(a, b, 1, 0)

def mm_nt(a, b):
    return dot(a, b, 1, 1)

def mm_tn(a, b):
    return dot(a, b, 0, 0)

def half_masks():
    lane = lax.broadcasted_iota(jnp.int32, (T, N), 1)
    sub = lax.broadcasted_iota(jnp.int32, (T, N), 0)
    left = lane < H
    return jnp.where(left, lane, lane - H), sub, jnp.where(left, 0, H)

def pick(x, base, c):
    return jnp.take_along_axis(x, base + c, axis=1, mode="promise_in_bounds")

def row_bcast(ref, row):
    return jnp.broadcast_to(ref[row : row + 1, :], (T, N))

def assemble(rows, k, col, sub):
    tile = rows[T - 1]
    for j in range(T - 2, -1, -1):
        tile = jnp.where(sub <= j, rows[j], tile)
    return jnp.where(col <= sub + k, tile, 0.0)

def chol_leaf(mat, sc, sl, sr, fill=()):
    fill = list(fill)
    rate = -(-len(fill) // NB)
    col, sub, base = half_masks()
    mat = list(mat)
    out = []
    own = [pick(mat[0], base, j) for j in range(T)]
    for b in range(NB):
        k = b * T
        inside = (col >= k) & (col < k + T)
        unit = (col == sub + k).astype(F32)
        cs, ls, rs = sc.at[b % 2], sl.at[b % 2], sr.at[b % 2]
        for j in range(T):
            cs[j * T : (j + 1) * T, :] = own[j]
        rs[...] = jnp.where(inside, unit, mat[b])
        a = {(i, j): row_bcast(cs, j * T + i) for j in range(T) for i in range(j, T)}
        r = [row_bcast(rs, j) for j in range(T)]
        below = range(b + 1, NB)
        c = {t: [pick(mat[t], base, k + j) for j in range(T)] for t in below}
        if b < NB - 1:
            own = [pick(mat[b + 1], base, k + T + j) for j in range(T)]
        acc = {t: jnp.where(inside, 0.0, mat[t]) for t in below}
        for task in fill[b * rate : (b + 1) * rate]:
            task()
        for j in range(T):
            scale = lax.rsqrt(a[j, j])
            low = {i: a[i, j] * scale for i in range(j + 1, T)}
            for i in range(j + 1, T):
                for i2 in range(j + 1, i + 1):
                    a[i, i2] = a[i, i2] - low[i] * low[i2]
            r[j] = r[j] * scale
            for i in range(j + 1, T):
                r[i] = r[i] - low[i] * r[j]
            for t in below:
                c[t][j] = c[t][j] * scale
                for i in range(j + 1, T):
                    c[t][i] = c[t][i] - low[i] * c[t][j]
                acc[t] = acc[t] - c[t][j] * r[j]
            if b < NB - 1:
                ls[j * T : (j + 1) * T, :] = c[b + 1][j]
                for i in range(T):
                    own[i] = own[i] - c[b + 1][j] * row_bcast(ls, j * T + i)
        out.append(assemble(r, k, col, sub))
        for t in below:
            mat[t] = acc[t]
    return out

def tri_leaf(mats, scs, srs):
    lane = lax.broadcasted_iota(jnp.int32, (T, N), 1)
    sub = lax.broadcasted_iota(jnp.int32, (T, N), 0)
    col = lane % SMALL
    base = lane - col
    count = SMALL // T
    outs = [[] for _ in mats]
    picks = []
    for mat, sc in zip(mats, scs):
        picks.append([{t: [pick(mat[t], base, b * T + j) for j in range(T)] for t in range(b, count)} for b in range(count)])
        for b in range(count):
            for j in range(T):
                sc[b, j * T : (j + 1) * T, :] = picks[-1][b][b][j]
    mats = [[jnp.zeros((T, N), F32) for _ in m] for m in mats]
    for b in range(count):
        k = b * T
        inside = (col >= k) & (col < k + T)
        unit = (col == sub + k).astype(F32)
        for q, mat in enumerate(mats):
            cs, rs = scs[q].at[b], srs[q].at[b % 2]
            rs[...] = jnp.where(inside, unit, mat[b])
            r = [row_bcast(rs, j) for j in range(T)]
            for j in range(T):
                r[j] = r[j] * (1.0 / row_bcast(cs, j * T + j))
                for i in range(j + 1, T):
                    r[i] = r[i] - row_bcast(cs, j * T + i) * r[j]
            outs[q].append(assemble(r, k, col, sub))
            for t in range(b + 1, count):
                for j in range(T):
                    mat[t] = mat[t] - picks[q][b][t][j] * r[j]
    return outs

def split_halves(x):
    lane = lax.broadcasted_iota(jnp.int32, x.shape, 1)
    return jnp.concatenate([jnp.where(lane < H, x, 0.0), jnp.where(lane < H, 0.0, x)], axis=0)

def pack(first, second):
    lane = lax.broadcasted_iota(jnp.int32, first.shape, 1)
    return (
        jnp.where(lane < H, first, pltpu.roll(second, H, 1)),
        jnp.where(lane < H, pltpu.roll(first, H, 1), second),
    )

def tiles_of(ref, r0, c0):
    return [ref[r0 + t * T : r0 + (t + 1) * T, c0 : c0 + N] for t in range(NB)]

def chol_inverse_pair(gram, inv, tmp, parts, sc, sl, sr, fills):
    n = gram.shape[0]
    nb = n // H
    rows = lambda e: slice(e * H, (e + 1) * H)
    cols = lambda e: slice(e * N, (e + 1) * N)
    span = lambda e, f: slice(e * N, f * N)
    pairs = lambda e, f: [(i, min(i + 2, f)) for i in range(e, f, 2)]

    def solve(d, at):
        tmp[at, cols(d)] = mm_nt(gram[at, cols(d)], split_halves(inv[rows(d), cols(d)]))

    def shrink(d, e, f, at):
        weights = jnp.concatenate([split_halves(tmp[rows(i), cols(d)]) for i in range(e, f)], axis=0)
        gram[at, span(e, f)] = gram[at, span(e, f)] - mm_nt(tmp[at, cols(d)], weights)

    def gather(d, e, f, c, b):
        weights = jnp.concatenate(
            [
                jnp.concatenate([split_halves(inv[rows(i), cols(k)]) for k in range(c, b)], axis=1)
                for i in range(e, f)
            ],
            axis=0,
        )
        part = mm(tmp[rows(d), span(e, f)], weights)
        parts[:, span(c, b)] = part if e == 0 else parts[:, span(c, b)] + part

    def finish(d, c, b):
        weights = jnp.concatenate([split_halves(parts[:, cols(k)]) for k in range(c, b)], axis=1)
        inv[rows(d), span(c, b)] = -mm(inv[rows(d), cols(d)], weights)

    inv[...] = jnp.zeros(inv.shape, F32)
    pending = []
    for d in range(nb):
        tasks = pending + [lambda e=e, f=f, c=c, b=b: gather(d, e, f, c, b) for e, f in pairs(0, d) for c, b in pairs(0, d)]
        tasks += fills.get(d, [])
        for t, tile in enumerate(chol_leaf(tiles_of(gram, d * H, d * N), sc, sl, sr, tasks)):
            inv[d * H + t * T : d * H + (t + 1) * T, cols(d)] = tile
        pending = []
        if d < nb - 1:
            solve(d, rows(d + 1))
            shrink(d, d + 1, d + 2, rows(d + 1))
            if d + 2 < nb:
                later = slice((d + 2) * H, n)
                pending.append(lambda d=d, at=later: solve(d, at))
                pending.append(lambda d=d, at=later: shrink(d, d + 1, d + 3, at))
            for e, f in pairs(d + 3, nb):
                pending.append(lambda d=d, e=e, f=f: shrink(d, e, f, slice(e * H, n)))
            pending += [lambda d=d, c=c, b=b: finish(d, c, b) for c, b in pairs(0, d)]
        else:
            for c, b in pairs(0, d):
                finish(d, c, b)

def unpack(inv, first, second):
    n = inv.shape[0]
    for c in range(0, n, N):
        first[:, c : c + N], second[:, c : c + N] = pack(inv[:, 2 * c : 2 * c + N], inv[:, 2 * c + N : 2 * c + 2 * N])

def tri_inverse(block, inverse, scs, srs):
    n = block.shape[0]
    lane = lax.broadcasted_iota(jnp.int32, (T, N), 1)
    mats = []
    for c in range(0, n, N):
        tiles = []
        for t in range(SMALL // T):
            tile = block[c + t * T : c + (t + 1) * T, c : c + N]
            for i in range(SMALL, N, SMALL):
                tile = jnp.where(lane < i, tile, block[c + i + t * T : c + i + (t + 1) * T, c : c + N])
            tiles.append(tile)
        mats.append(tiles)
    outs = tri_leaf(mats, scs, srs)
    row = lax.broadcasted_iota(jnp.int32, (N, N), 0)
    col = lax.broadcasted_iota(jnp.int32, (N, N), 1)
    for c, out in zip(range(0, n, N), outs):
        for i in range(0, N, SMALL):
            for t, tile in enumerate(out):
                inverse[c + i + t * T : c + i + (t + 1) * T, c : c + N] = jnp.where(
                    (lane >= i) & (lane < i + SMALL), tile, 0.0
                )
    for c in range(0, n, N):
        value = inverse[c : c + N, c : c + N]
        size = SMALL
        while size < N:
            corner = (row // size == col // size + 1) & (row // size % 2 == 1)
            value = value - mm(value, mm(jnp.where(corner, block[c : c + N, c : c + N], 0.0), value))
            size *= 2
        inverse[c : c + N, c : c + N] = value


def inverse_kernel(flags, factor, inverse, scs, srs):
    width = inverse.shape[0]
    block = factor.at[:, pl.ds(pl.multiple_of(flags[0] * width, width), width)]
    tri_inverse(block, inverse, [scs.at[q] for q in range(2)], [srs.at[q] for q in range(2)])


def solve_kernel(flags, factor, update, inverse, left, right, rhs):
    width = update.shape[1]
    half = width // 2
    block = factor.at[:, pl.ds(pl.multiple_of(flags[0] * width, width), width)]
    for c in range(0, width, N):
        at = slice(c, c + N)
        inv = inverse[at, at]
        for source, low in ((update, 0), (factor, width)):
            value = source[at, :width]
            if c > 0:
                value = value - mm(block[at, :c], rhs[:c, low : low + width])
            rhs[at, low : low + width] = mm(inv, value)
    for out, low in ((left, 0), (right, half)):
        out[:, :half] = rhs[:, low : low + half]
        out[:, half:] = rhs[:, width + low : width + low + half]


def gram_rows(g, gram, low, high, width):
    row = lax.broadcasted_iota(jnp.int32, (high - low, width), 0) + low
    eye = (row == lax.broadcasted_iota(jnp.int32, (high - low, width), 1)).astype(F32)
    first = eye + mm_nt(g[low:high, :], g[:width, :])
    left = g[:, :N] if high <= N else g[...]
    second = eye + mm_tn(left, g[:, :width])[low:high, :]
    for c in range(0, width, N):
        gram[low:high, 2 * c : 2 * c + N], gram[low:high, 2 * c + N : 2 * c + 2 * N] = pack(
            first[:, c : c + N], second[:, c : c + N]
        )


def update_kernel(
    flags, factor, update, own, other, own_swapped, other_swapped,
    new_factor, new_update, copies, g, x, y, mixed, current, inv_l, inv_c, gram, inv, tmp, parts, sc, sl, sr,
):
    width = g.shape[0]
    half = width // 2
    panels = factor.shape[1] // width
    south = flags[1] == 1
    odd = flags[2] == 1
    part = lambda p: slice(p * width, (p + 1) * width)

    def halves(out, low, swap):
        at = slice(low, low + half)
        here = jnp.where(odd != swap, other[:, at], own[:, at])
        there = jnp.where(odd != swap, other_swapped[:, at], own_swapped[:, at])
        out[:, :half] = jnp.where(south, there, here)
        out[:, half:] = jnp.where(south, here, there)

    def mix(p):
        v = update if p == 0 else new_update
        mixed[...] = factor[:, part(p)] + mm_nt(v[...], g[...])

    def lower(p):
        v = update if p == 0 else new_update
        current[...] = v[...] - mm(factor[:, part(p)], g[...])

    def carry():
        x[...] = x[...] - mm(y[...], g[...])

    def columns(p):
        new_factor[:, part(p)] = mm_nt(mixed[...], inv_l[...])

    def updates():
        new_update[...] = mm_nt(current[...], inv_c[...])

    halves(g, 0, False)
    halves(y, half, True)
    halves(x, 0, True)
    held = []
    for p in range(panels):
        gram_rows(g, gram, 0, H, N)
        rest = [lambda: gram_rows(g, gram, H, width, width)]
        tasks = {0: rest + held, 1: [lambda: mix(p), lambda: lower(p)], 2: [carry] if p < panels - 1 else []}
        chol_inverse_pair(gram, inv, tmp, parts, sc, sl, sr, tasks)
        unpack(inv, inv_l, inv_c)
        held = [lambda p=p: columns(p), updates]
        if p < panels - 1:
            g[...] = mm_nt(x[...], inv_c[...])
    for task in held:
        task()
    squares = jnp.sum(new_factor[...] * new_factor[...], axis=0, keepdims=True)
    copies[...] = jnp.broadcast_to(squares, copies.shape)


def masks_of(rows, cols):
    bits = lambda low, high: [1 << b for b in range(high.bit_length() - 2, low.bit_length() - 2, -1)]
    return cols, bits(2, cols) + bits(2 * cols, rows * cols)


def spread(left, right, my_index, core, steps, roots):
    turned = steps[-1:] + steps[:-1]
    steps = steps[:1] + steps[-1:] + steps[1:-1]
    sent = lax.ppermute(right, AXES, [(d, d | core) for d in roots])
    part = jnp.where((my_index & core) != 0, sent, left)
    seen = [set(roots), {core | d for d in roots}]
    for step in range(len(steps)):
        pairs = []
        for side, order in ((0, steps), (1, turned)):
            new = {(d, d ^ order[step]) for d in seen[side]}
            pairs += sorted(new)
            seen[side] |= {d for _, d in new}
        came = lax.ppermute(part, AXES, pairs)
        target = jnp.zeros((), bool)
        for _, d in pairs:
            target = target | (my_index == d)
        part = jnp.where(target, came, part)
    return part


def on_device(factor, update):
    rows, cols_count = lax.axis_size("row"), lax.axis_size("col")
    total = rows * cols_count
    my_index = lax.axis_index(AXES)
    tile, wide = factor.shape[1], factor.shape[2]
    width = update.shape[2]
    panels = wide // width
    flat_factor = factor.reshape(tile, wide)
    flat_update = update.reshape(tile, width)
    core, others = masks_of(rows, cols_count)
    panel = jnp.minimum(my_index & ~core, panels - 1)
    flags = jnp.stack([panel, jnp.minimum(my_index & core, 1), my_index & 1]).astype(jnp.int32)
    smem = pl.BlockSpec(memory_space=pltpu.SMEM)
    vmem = pl.BlockSpec(memory_space=pltpu.VMEM)
    shape = lambda *dims: jax.ShapeDtypeStruct(dims, F32)
    work = lambda *dims: pltpu.VMEM(dims, F32)
    limit = pltpu.CompilerParams(vmem_limit_bytes=24 * 2 ** 20)

    blocks = width // N
    inverse = pl.pallas_call(
        inverse_kernel,
        out_shape=shape(width, width),
        in_specs=[smem, vmem],
        out_specs=vmem,
        scratch_shapes=[work(blocks, NB, T * T, N), work(blocks, 2, T, N)],
        compiler_params=limit,
        name="inverse",
    )(flags, flat_factor)
    left, right = pl.pallas_call(
        solve_kernel,
        out_shape=(shape(width, width),) * 2,
        in_specs=[smem] + [vmem] * 3,
        out_specs=(vmem,) * 2,
        scratch_shapes=[work(width, 2 * width)],
        compiler_params=limit,
        name="solve",
    )(flags, flat_factor, flat_update, inverse)
    own = spread(left, right, my_index, core, others, (0, 1))
    partner = [(d, d ^ core) for d in range(total)]
    other = lax.ppermute(own, AXES, [(d, d ^ 1) for d in range(total)])
    own_swapped = lax.ppermute(own, AXES, partner)
    other_swapped = lax.ppermute(other, AXES, partner)
    new_factor, new_update, copies = pl.pallas_call(
        update_kernel,
        out_shape=(shape(tile, wide), shape(tile, width), shape(total, wide)),
        in_specs=[smem] + [vmem] * 6,
        out_specs=(vmem,) * 3,
        scratch_shapes=[work(width, width)] * 3
        + [work(tile, width)] * 2
        + [work(width, width)] * 2
        + [work(width, 2 * width)] * 3
        + [work(H, 2 * width), work(2, T * T, N), work(2, T * T, N), work(2, T, N)],
        compiler_params=limit,
        cost_estimate=pl.CostEstimate(flops=10 ** 10, bytes_accessed=2 ** 21, transcendentals=0),
        name="update",
    )(flags, flat_factor, flat_update, own, other, own_swapped, other_swapped)
    gathered = lax.all_to_all(copies, AXES, 0, 0, tiled=True)
    squares = jnp.sum(gathered, axis=0)
    column_scale = jnp.sqrt(squares / (tile * total) + 1e-06)
    return (new_factor.reshape(factor.shape), new_update.reshape(update.shape), column_scale)


def solution(mesh):
    return jax.shard_map(
        on_device,
        mesh=mesh,
        in_specs=(P(None, AXES, None), P(None, AXES, None)),
        out_specs=(P(None, AXES, None), P(None, AXES, None), P()),
        check_vma=False,
    )
```
